32 devices in a mesh: dp: 8 (over z, x), tensor: 4 (over y, core).
Axes of the slice: x: 2, y: 2, z: 4, core: 2. Of those that a mesh axis runs over, the one named last changes fastest.
Arguments:
- tokens: bfloat16 [16384, 1536], P(('dp', 'tensor')), may hold values from -6 to 6
- attn_gain: bfloat16 [1536], P('dp'), may hold values from 0.5 to 1.5
- w_query: bfloat16 [1536, 1536], P('dp', 'tensor'), may hold values from -0.15625 to 0.15625
- w_key: bfloat16 [1536, 1536], P('dp', 'tensor'), may hold values from -0.15625 to 0.15625
- w_value: bfloat16 [1536, 1536], P('dp', 'tensor'), may hold values from -0.15625 to 0.15625
- w_outgate: bfloat16 [1536, 1536], P('dp', 'tensor'), may hold values from -0.15625 to 0.15625
- w_forget: bfloat16 [1536, 24], P('dp', 'tensor'), may hold values from -0.15625 to 0.15625
- forget_bias: float32 [24], replicated, may hold values from 0.5 to 7
- w_output: bfloat16 [1536, 1536], P('tensor', 'dp'), may hold values from -0.875 to 0.875
- query_gain: bfloat16 [64], replicated, may hold values from 0.25 to 1.75
- key_gain: bfloat16 [64], replicated, may hold values from 0.25 to 1.75
- mlp_gain: bfloat16 [1536], P('dp'), may hold values from 0.5 to 1.5
- w_gate: bfloat16 [1536, 4096], P('dp', 'tensor'), may hold values from -0.15625 to 0.15625
- w_up: bfloat16 [1536, 4096], P('dp', 'tensor'), may hold values from -0.15625 to 0.15625
- w_down: bfloat16 [4096, 1536], P('tensor', 'dp'), may hold values from -0.125 to 0.125
- lengths: int32 [8], P('dp'), may hold values from 512 to 2048, as said below
- out_grad: bfloat16 [16384, 1536], P(('dp', 'tensor')), may hold values from -6 to 6
Outputs:
- mixed_out: bfloat16 [16384, 1536], P(('dp', 'tensor'))
- tokens_grad: float32 [16384, 1536], P(('dp', 'tensor'))
- attn_gain_grad: float32 [1536], P('dp')
- w_query_grad: float32 [1536, 1536], P('dp', 'tensor')
- w_key_grad: float32 [1536, 1536], P('dp', 'tensor')
- w_value_grad: float32 [1536, 1536], P('dp', 'tensor')
- w_outgate_grad: float32 [1536, 1536], P('dp', 'tensor')
- w_forget_grad: float32 [1536, 24], P('dp', 'tensor')
- forget_bias_grad: float32 [24], replicated
- w_output_grad: float32 [1536, 1536], P('tensor', 'dp')
- query_gain_grad: float32 [64], replicated
- key_gain_grad: float32 [64], replicated
- mlp_gain_grad: float32 [1536], P('dp')
- w_gate_grad: float32 [1536, 4096], P('dp', 'tensor')
- w_up_grad: float32 [1536, 4096], P('dp', 'tensor')
- w_down_grad: float32 [4096, 1536], P('tensor', 'dp')
The draws below stay inside these ranges and needn't reach their ends.
Inputs may be any that keep to these rules, and one draw needn't show every extreme that they name: `lengths`: in every draw one slot holds exactly 2048 live tokens and another exactly 512.
All inputs are finite; a program needn't handle non-finite values.
Results may differ from the reference program's by a relative error of at most 0.018.
Values may be sent and summed in bfloat16 or wider, within the bound.
A program may use at most 256 MiB of HBM per device.

```python
import jax
import jax.numpy as jnp
from jax import lax

D = 1536
HEADS = 24
HEAD_DIM = 64
FF = 4096
SLOT = 2048
MIN_LEN = 512
SLOTS = 8
TOKENS = 16384


def draw_lengths(key, part):
    base = jax.random.randint(jax.random.fold_in(key, 11), (SLOTS,), MIN_LEN, SLOT + 1)
    order = jax.random.permutation(jax.random.fold_in(key, 12), SLOTS)
    places = jnp.arange(SLOTS)
    base = jnp.where(places == order[0], SLOT, base)
    base = jnp.where(places == order[1], MIN_LEN, base)
    return base.astype(jnp.int32)


def strengthened(drawn, stream_key, source, target, parts, factor):
    owner, partner = [(jnp.arange(drawn.shape[axis_at]) // (drawn.shape[axis_at] // parts)).reshape([-1 if axis == axis_at else 1 for axis in range(drawn.ndim)]) for axis_at in (source, target)]
    chosen = jax.random.permutation(stream_key, parts)[partner]
    strong = (owner == chosen) | (owner == (partner + parts // 2) % parts)
    return jnp.where(strong, factor * drawn, drawn)


def steps_of(key, extent, shards, least, high):
    def one(axis_at, blocks):
        steps = jax.random.uniform(jax.random.fold_in(jax.random.fold_in(key, 6), axis_at), (blocks,), jnp.float32, least / len(shards), high / len(shards))
        return jnp.repeat(jnp.exp(steps), extent[axis_at] // blocks).reshape((-1,) + (1,) * (len(extent) - axis_at - 1))

    factor_of = one(*shards[0])
    for cut in shards[1:]:
        factor_of = factor_of * one(*cut)
    return factor_of


def noise(own_key, shape, width, limit, split=(), held_as=jnp.bfloat16):
    result = width * jax.random.normal(own_key, shape, jnp.float32)
    if split:
        result = result * steps_of(own_key, shape, split, -0.22, 0.18)
    return jnp.clip(result, -limit, limit).astype(held_as)


def noise_with(rng, extent, width, most, pieces, heavy, kind=jnp.bfloat16):
    array = width * jax.random.normal(rng, extent, jnp.float32)
    if pieces:
        array = array * steps_of(rng, extent, pieces, -0.22, 0.18)
    return jnp.clip(strengthened(array, jax.random.fold_in(rng, 3), *heavy), -most, most).astype(kind)


def setup_inputs(seed: int = 0) -> dict:
    streams_of = jax.random.split(jax.random.key(seed), 18)
    tokens = noise_with(streams_of[0], (TOKENS, D), 1.0, 6.0, ((0, 32),), (0, 1, 32, 2.75))
    attn_gain = jnp.clip(1.0 + 0.1 * jax.random.normal(streams_of[1], (D,), jnp.float32), 0.5, 1.5).astype(jnp.bfloat16)
    w_query = noise(streams_of[2], (D, HEADS * HEAD_DIM), D ** -0.5, 0.15625, ((0, 8), (1, 4)))
    w_key = noise(streams_of[3], (D, HEADS * HEAD_DIM), D ** -0.5, 0.15625, ((0, 8), (1, 4)))
    w_value = noise(streams_of[4], (D, HEADS * HEAD_DIM), D ** -0.5, 0.15625, ((0, 8), (1, 4)))
    w_outgate = noise(streams_of[5], (D, HEADS * HEAD_DIM), D ** -0.5, 0.15625, ((0, 8), (1, 4)))
    w_forget = noise(streams_of[6], (D, HEADS), D ** -0.5, 0.15625, ((0, 8), (1, 4)))
    forget_bias = jnp.clip(jax.random.uniform(streams_of[7], (HEADS,), jnp.float32, 0.5, 7.0), 0.5, 7.0)
    w_output = noise(streams_of[8], (HEADS * HEAD_DIM, D), (HEADS * HEAD_DIM // 32) ** -0.5, 0.875, ((0, 4), (1, 8)))
    query_gain = jnp.clip(1.0 + 0.15 * jax.random.normal(streams_of[9], (HEAD_DIM,), jnp.float32), 0.25, 1.75).astype(jnp.bfloat16)
    key_gain = jnp.clip(1.0 + 0.15 * jax.random.normal(streams_of[10], (HEAD_DIM,), jnp.float32), 0.25, 1.75).astype(jnp.bfloat16)
    mlp_gain = jnp.clip(1.0 + 0.1 * jax.random.normal(streams_of[11], (D,), jnp.float32), 0.5, 1.5).astype(jnp.bfloat16)
    w_gate = noise(streams_of[12], (D, FF), D ** -0.5, 0.15625, ((0, 8), (1, 4)))
    w_up = noise(streams_of[13], (D, FF), D ** -0.5, 0.15625, ((0, 8), (1, 4)))
    w_down = noise(streams_of[14], (FF, D), (FF // 2) ** -0.5, 0.125, ((0, 4), (1, 8)))
    lengths = draw_lengths(jax.random.fold_in(streams_of[17], 71), 0)
    out_grad = noise_with(streams_of[16], (TOKENS, D), 1.0, 6.0, ((0, 32),), (0, 1, 32, 2.75))
    return {"tokens": tokens, "attn_gain": attn_gain, "w_query": w_query, "w_key": w_key, "w_value": w_value, "w_outgate": w_outgate, "w_forget": w_forget, "forget_bias": forget_bias, "w_output": w_output, "query_gain": query_gain, "key_gain": key_gain, "mlp_gain": mlp_gain, "w_gate": w_gate, "w_up": w_up, "w_down": w_down, "lengths": lengths, "out_grad": out_grad}


@jax.custom_vjp
def low(v):
    return lax.optimization_barrier(v.astype(jnp.bfloat16)).astype(jnp.float32)

@jax.custom_vjp
def low_back(v):
    return v

def low_keep(v):
    return (low(v), None)

def low_pass(kept, grad):
    return (grad,)

def back_keep(v):
    return (v, None)

def back_low(kept, grad):
    return (low(grad),)
low.defvjp(low_keep, low_pass)
low_back.defvjp(back_keep, back_low)
EPSILON = 1e-05
NEGATIVE = -1e+30

def highest(left, right):
    return jnp.dot(left, right, precision=lax.Precision.HIGHEST, preferred_element_type=jnp.float32)

def rms_scale(values):
    return lax.rsqrt(lax.optimization_barrier(jnp.mean(values * values, axis=-1, keepdims=True)) + EPSILON)

def slot_forward(params, slot_rows, slot_length):
    attn_gain, w_query, w_key, w_value, w_outgate, w_forget, forget_bias, w_output, query_gain, key_gain, mlp_gain, w_gate, w_up, w_down = params
    normed = low(slot_rows * rms_scale(slot_rows) * attn_gain)
    query_raw = low_back(highest(normed, w_query)).reshape(SLOT, HEADS, HEAD_DIM)
    key_raw = low_back(highest(normed, w_key)).reshape(SLOT, HEADS, HEAD_DIM)
    value_low = low(low_back(highest(normed, w_value))).reshape(SLOT, HEADS, HEAD_DIM)
    gate_logit = low_back(highest(normed, w_outgate))
    forget_logit = low_back(highest(normed, w_forget) + forget_bias)
    query_low = low(query_raw * rms_scale(query_raw) * query_gain)
    key_low = low(key_raw * rms_scale(key_raw) * key_gain)
    cumulative = jnp.cumsum(jax.nn.log_sigmoid(forget_logit), axis=0)
    positions = jnp.arange(SLOT)
    allowed = (positions[None, :] <= positions[:, None]) & (positions < slot_length)[None, :]
    scores = jnp.einsum('qhd,khd->hqk', query_low, key_low, precision=lax.Precision.HIGHEST, preferred_element_type=jnp.float32) * HEAD_DIM ** (-0.5)
    scores = scores + jnp.transpose(cumulative)[:, :, None] - jnp.transpose(cumulative)[:, None, :]
    scores = low_back(jnp.where(allowed[None], scores, NEGATIVE))
    probs_low = low(jax.nn.softmax(scores, axis=-1))
    attended = low_back(jnp.einsum('hqk,khd->qhd', probs_low, value_low, precision=lax.Precision.HIGHEST, preferred_element_type=jnp.float32))
    gated = low(attended.reshape(SLOT, HEADS * HEAD_DIM) * jax.nn.sigmoid(gate_logit))
    mixed = slot_rows + low_back(highest(gated, w_output))
    normed_mid = low(mixed * rms_scale(mixed) * mlp_gain)
    gate_value = low_back(highest(normed_mid, w_gate))
    up_value = low_back(highest(normed_mid, w_up))
    hidden = low(jax.nn.silu(gate_value) * up_value)
    return mixed + highest(hidden, w_down)

def reference(tokens, attn_gain, w_query, w_key, w_value, w_outgate, w_forget, forget_bias, w_output, query_gain, key_gain, mlp_gain, w_gate, w_up, w_down, lengths, out_grad):
    params = (attn_gain.astype(jnp.float32), w_query.astype(jnp.float32), w_key.astype(jnp.float32), w_value.astype(jnp.float32), w_outgate.astype(jnp.float32), w_forget.astype(jnp.float32), forget_bias.astype(jnp.float32), w_output.astype(jnp.float32), query_gain.astype(jnp.float32), key_gain.astype(jnp.float32), mlp_gain.astype(jnp.float32), w_gate.astype(jnp.float32), w_up.astype(jnp.float32), w_down.astype(jnp.float32))
    slot_rows = tokens.astype(jnp.float32).reshape(SLOTS, SLOT, D)

    def forward(params_in, rows_in):

        def one_slot(packed):
            return slot_forward(params_in, packed[0], packed[1])
        return lax.map(jax.checkpoint(one_slot), (rows_in, lengths))
    outputs, pullback = jax.vjp(forward, params, slot_rows)
    positions = jnp.arange(SLOT)
    live_rows = (positions[None, :] < lengths[:, None]).astype(jnp.float32)
    cotangent = out_grad.astype(jnp.float32).reshape(SLOTS, SLOT, D) * live_rows[:, :, None]
    param_grads, row_grads = pullback(cotangent)
    return (outputs.reshape(TOKENS, D).astype(jnp.bfloat16), row_grads.reshape(TOKENS, D), param_grads[0], param_grads[1], param_grads[2], param_grads[3], param_grads[4], param_grads[5], param_grads[6], param_grads[7], param_grads[8], param_grads[9], param_grads[10], param_grads[11], param_grads[12], param_grads[13])
```

```python
import functools
import math

import jax
import jax.numpy as jnp
from jax import lax
from jax.experimental import pallas as pl
from jax.experimental.pallas import tpu as pltpu
from jax.sharding import PartitionSpec as P

NEGATIVE = -1e30
EPSILON = 1e-05


def nt(left, right):
    return lax.dot_general(
        left, right, (((1,), (1,)), ((), ())), preferred_element_type=jnp.float32
    )


def tn(left, right):
    return lax.dot_general(
        left, right, (((0,), (0,)), ((), ())), preferred_element_type=jnp.float32
    )


def nn(left, right):
    return jnp.dot(left, right, preferred_element_type=jnp.float32)


def split_three(values):
    high = values.astype(jnp.bfloat16).astype(jnp.float32)
    rest = values - high
    middle = rest.astype(jnp.bfloat16).astype(jnp.float32)
    return high, middle, rest - middle


def placed_pieces(values, lane, first):
    high, middle, low = split_three(values)
    return jnp.where(
        lane == first, high, jnp.where(lane == first + 1, middle, jnp.where(lane == first + 2, low, 0.0))
    )


def turned(values, head, half):
    return values if head == 0 else pltpu.roll(values, half, 1)


def attend_kernel(
    heads, half, block, x_ref, cq_ref, ck_ref, qg_ref, kg_ref, att_ref, qb_ref, kf_ref, qf, vf
):
    pair = pl.program_id(0)
    slot = x_ref.shape[0]
    wide = 2 * half
    blocks = slot // block
    lane = lax.broadcasted_iota(jnp.int32, (block, wide), 1)
    lower = lane < half
    row = lax.broadcasted_iota(jnp.int32, (wide, wide), 0)
    col = lax.broadcasted_iota(jnp.int32, (wide, wide), 1)
    below = lax.broadcasted_iota(jnp.int32, (block, block), 0) >= lax.broadcasted_iota(
        jnp.int32, (block, block), 1
    )
    for h in range(2):
        head = pair * 2 + h
        place_q = ((row == (col - half) * heads + head) & (col >= half) & (col < half + 3)).astype(
            jnp.bfloat16
        )
        place_k = (
            (row == (col - half - 3) * heads + head) & (col >= half + 3) & (col < half + 6)
        ).astype(jnp.bfloat16)

        def prepare(b, _):
            rows = pl.ds(pl.multiple_of(b * block, block), block)
            q = turned(x_ref[rows, 0:wide], h, half)
            k = turned(x_ref[rows, wide : 2 * wide], h, half)
            v = turned(x_ref[rows, 2 * wide : 3 * wide], h, half)
            q_scale = lax.rsqrt(
                jnp.sum(jnp.where(lower, q * q, 0.0), axis=1, keepdims=True) / half + EPSILON
            )
            k_scale = lax.rsqrt(
                jnp.sum(jnp.where(lower, k * k, 0.0), axis=1, keepdims=True) / half + EPSILON
            )
            q_low = (q * q_scale * qg_ref[...]).astype(jnp.bfloat16).astype(jnp.float32)
            k_low = k * k_scale * kg_ref[...]
            q_bias = nn(cq_ref[rows, :], place_q) + jnp.where(
                (lane >= half + 3) & (lane < half + 6), 1.0, 0.0
            )
            k_bias = nn(ck_ref[rows, :], place_k) + jnp.where(
                (lane >= half) & (lane < half + 3), 1.0, 0.0
            )
            qf[rows, :] = jnp.where(lower, q_low * (1.0 / math.sqrt(half)), q_bias).astype(
                jnp.bfloat16
            )
            kf_ref[h, rows, :] = jnp.where(lower, k_low, k_bias).astype(jnp.bfloat16)
            vf[rows, :] = jnp.where(lower, v, 1.0).astype(jnp.bfloat16)
            return 0

        lax.fori_loop(0, blocks, prepare, 0)
        for qb in range(blocks):
            rows = pl.ds(qb * block, block)
            query = qf[rows, :]
            total = jnp.zeros((block, wide), jnp.float32)
            for kb in range(qb + 1):
                keys = pl.ds(kb * block, block)
                scores = nt(query, kf_ref[h, keys, :])
                if kb == qb:
                    scores = jnp.where(below, scores, NEGATIVE)
                total = total + nn(jnp.exp(scores).astype(jnp.bfloat16), vf[keys, :])
            out = total / pltpu.roll(total, half, 1)
            if h == 0:
                att_ref[rows, :] = out
            else:
                att_ref[rows, :] = jnp.where(lower, att_ref[rows, :], pltpu.roll(out, half, 1))
            query_float = query.astype(jnp.float32)
            bias = jnp.sum(
                jnp.where((lane >= half) & (lane < half + 3), query_float, 0.0),
                axis=1,
                keepdims=True,
            )
            shifted = bias - jnp.log(jnp.where(lower, 1.0, total))
            qb_ref[h, rows, :] = jnp.where(
                (lane >= half) & (lane < half + 3),
                placed_pieces(shifted, lane, half),
                query_float,
            ).astype(jnp.bfloat16)


def attend_back_kernel(
    half,
    block,
    x_ref,
    qb_ref,
    kf_ref,
    att_ref,
    do_ref,
    qg_ref,
    kg_ref,
    grad_ref,
    cum_ref,
    gain_ref,
    vf,
    dof,
    key_turned,
    dq_turned,
    dk_all,
    dv_all,
):
    pair = pl.program_id(0)
    slot = x_ref.shape[0]
    wide = 2 * half
    blocks = slot // block
    lane = lax.broadcasted_iota(jnp.int32, (block, wide), 1)
    lower = lane < half
    above = lax.broadcasted_iota(jnp.int32, (block, block), 0) <= lax.broadcasted_iota(
        jnp.int32, (block, block), 1
    )

    @pl.when(pair == 0)
    def _():
        gain_ref[...] = jnp.zeros_like(gain_ref)
        cum_ref[...] = jnp.zeros_like(cum_ref)

    for h in range(2):
        head = pair * 2 + h

        def prepare(b, _):
            rows = pl.ds(pl.multiple_of(b * block, block), block)
            v = turned(x_ref[rows, 2 * wide : 3 * wide], h, half)
            grad = turned(do_ref[rows, :].astype(jnp.float32), h, half)
            out = turned(att_ref[rows, :], h, half)
            inner = jnp.sum(jnp.where(lower, grad * out, 0.0), axis=1, keepdims=True)
            vf[rows, :] = jnp.where(lower, v, 1.0).astype(jnp.bfloat16)
            dof[rows, :] = jnp.where(lower, grad, placed_pieces(-inner, lane, half)).astype(
                jnp.bfloat16
            )
            key_turned[:, rows] = kf_ref[h, rows, :].astype(jnp.float32).T.astype(jnp.bfloat16)
            return 0

        lax.fori_loop(0, blocks, prepare, 0)
        for kb in range(blocks):
            keys = pl.ds(kb * block, block)
            key = kf_ref[h, keys, :]
            value = vf[keys, :]
            dk = jnp.zeros((block, wide), jnp.float32)
            dv = jnp.zeros((block, wide), jnp.float32)
            for qb in range(kb, blocks):
                rows = pl.ds(qb * block, block)
                query = qb_ref[h, rows, :]
                grad = dof[rows, :]
                scores = nt(key, query)
                if kb == qb:
                    scores = jnp.where(above, scores, NEGATIVE)
                probs = jnp.exp(scores)
                dv = dv + nn(probs.astype(jnp.bfloat16), grad)
                grad_scores = (probs * nt(value, grad)).astype(jnp.bfloat16)
                dk = dk + nn(grad_scores, query)
                part = nn(key_turned[:, keys], grad_scores)
                if kb == 0:
                    dq_turned[:, rows] = part
                else:
                    dq_turned[:, rows] += part
            dk_all[keys, :] = dk
            dv_all[keys, :] = dv

        def finish(b, sums):
            rows = pl.ds(pl.multiple_of(b * block, block), block)
            dq = dq_turned[:, rows].T
            dk = dk_all[rows, :]
            change = jnp.sum(
                jnp.where(lane == half, dq - pltpu.roll(dk, wide - 3, 1), 0.0),
                axis=1,
                keepdims=True,
            )
            cum_ref[rows, :] = jnp.where(lane == head, change, cum_ref[rows, :])

            def one(raw, grad, gain):
                scale = lax.rsqrt(
                    jnp.sum(jnp.where(lower, raw * raw, 0.0), axis=1, keepdims=True) / half
                    + EPSILON
                )
                inward = grad * gain
                mean = (
                    jnp.sum(jnp.where(lower, inward * raw, 0.0), axis=1, keepdims=True) / half
                )
                out = scale * inward - raw * (scale * scale * scale) * mean
                return out, jnp.sum(grad * raw * scale, axis=0, keepdims=True)

            q_out, q_sum = one(
                turned(x_ref[rows, 0:wide], h, half), dq * (1.0 / math.sqrt(half)), qg_ref[...]
            )
            k_out, k_sum = one(turned(x_ref[rows, wide : 2 * wide], h, half), dk, kg_ref[...])
            v_out = dv_all[rows, :]
            for i, out in enumerate((q_out, k_out, v_out)):
                at = slice(i * wide, (i + 1) * wide)
                if h == 0:
                    grad_ref[rows, at] = out.astype(jnp.bfloat16)
                else:
                    grad_ref[rows, at] = jnp.where(
                        lower, grad_ref[rows, at].astype(jnp.float32), pltpu.roll(out, half, 1)
                    ).astype(jnp.bfloat16)
            return sums[0] + q_sum, sums[1] + k_sum

        zero = jnp.zeros((1, wide), jnp.float32)
        q_sum, k_sum = lax.fori_loop(0, blocks, finish, (zero, zero))
        gain_ref[0:1, :] += q_sum
        gain_ref[1:2, :] += k_sum


def attend(x, cq, ck, q_gain, k_gain, heads, half):
    slot = x.shape[0]
    wide = 2 * half
    pairs = heads // 2
    block = min(512, slot)
    constant = lambda rows: pl.BlockSpec((rows, wide), lambda j: (0, 0))
    area = slot * (slot + block) // 2
    return pl.pallas_call(
        functools.partial(attend_kernel, heads, half, block),
        grid=(pairs,),
        in_specs=[
            pl.BlockSpec((slot, 3 * wide), lambda j: (0, j)),
            constant(slot),
            constant(slot),
            constant(1),
            constant(1),
        ],
        out_specs=[
            pl.BlockSpec((slot, wide), lambda j: (0, j)),
            pl.BlockSpec((2, slot, wide), lambda j: (j, 0, 0)),
            pl.BlockSpec((2, slot, wide), lambda j: (j, 0, 0)),
        ],
        out_shape=[
            jax.ShapeDtypeStruct((slot, pairs * wide), jnp.float32),
            jax.ShapeDtypeStruct((heads, slot, wide), jnp.bfloat16),
            jax.ShapeDtypeStruct((heads, slot, wide), jnp.bfloat16),
        ],
        scratch_shapes=[pltpu.VMEM((slot, wide), jnp.bfloat16)] * 2,
        cost_estimate=pl.CostEstimate(
            flops=4 * heads * area * wide,
            transcendentals=heads * area,
            bytes_accessed=slot * pairs * wide * 24,
        ),
        name="attend",
    )(x, cq, ck, q_gain, k_gain)


def attend_back(x, qb, kf, att, grad, q_gain, k_gain, heads, half):
    slot = x.shape[0]
    wide = 2 * half
    pairs = heads // 2
    block = min(512, slot)
    area = slot * (slot + block) // 2
    gain = pl.BlockSpec((1, wide), lambda j: (0, 0))
    tall = pl.BlockSpec((2, slot, wide), lambda j: (j, 0, 0))
    column = pl.BlockSpec((slot, wide), lambda j: (0, j))
    return pl.pallas_call(
        functools.partial(attend_back_kernel, half, block),
        grid=(pairs,),
        in_specs=[
            pl.BlockSpec((slot, 3 * wide), lambda j: (0, j)),
            tall,
            tall,
            column,
            column,
            gain,
            gain,
        ],
        out_specs=[
            pl.BlockSpec((slot, 3 * wide), lambda j: (0, j)),
            pl.BlockSpec((slot, wide), lambda j: (0, 0)),
            pl.BlockSpec((8, wide), lambda j: (0, 0)),
        ],
        out_shape=[
            jax.ShapeDtypeStruct((slot, 3 * pairs * wide), jnp.bfloat16),
            jax.ShapeDtypeStruct((slot, wide), jnp.float32),
            jax.ShapeDtypeStruct((8, wide), jnp.float32),
        ],
        scratch_shapes=[
            pltpu.VMEM((slot, wide), jnp.bfloat16),
            pltpu.VMEM((slot, wide), jnp.bfloat16),
            pltpu.VMEM((wide, slot), jnp.bfloat16),
            pltpu.VMEM((wide, slot), jnp.float32),
            pltpu.VMEM((slot, wide), jnp.float32),
            pltpu.VMEM((slot, wide), jnp.float32),
        ],
        cost_estimate=pl.CostEstimate(
            flops=10 * heads * area * wide,
            transcendentals=heads * area,
            bytes_accessed=slot * pairs * wide * 40,
        ),
        name="attend_back",
    )(x, qb, kf, att, grad, q_gain, k_gain)


def split_pieces(values):
    high = lax.reduce_precision(values, 8, 7)
    middle = lax.reduce_precision(values - high, 8, 7)
    return high, middle, lax.reduce_precision(values - high - middle, 8, 7)


def bias_pieces(cumulative, length, slot, heads, wide):
    live = (jnp.arange(slot) < length)[:, None]
    last = lax.dynamic_slice_in_dim(cumulative, length - 1, 1, 0)
    query_side = jnp.where(live, cumulative, last)
    pad = jnp.zeros((slot, wide - 3 * heads), jnp.float32)
    high, middle, low = split_pieces(-cumulative)
    key_side = (jnp.where(live, high, NEGATIVE), jnp.where(live, middle, 0.0), jnp.where(live, low, 0.0))
    return (
        jnp.concatenate(split_pieces(query_side) + (pad,), axis=1).astype(jnp.bfloat16),
        jnp.concatenate(key_side + (pad,), axis=1).astype(jnp.bfloat16),
    )


def rms_scale(values):
    return lax.rsqrt(jnp.mean(values * values, axis=-1, keepdims=True) + EPSILON)


def norm_backward(values, scaling, grad_normed):
    cubed = scaling * scaling * scaling
    return scaling * grad_normed - values * cubed * jnp.mean(
        grad_normed * values, axis=-1, keepdims=True
    )


def gather(values, axis_name):
    return lax.all_gather(values, axis_name, axis=0, tiled=True)


def scatter(values, axis_name):
    return lax.psum_scatter(
        values.astype(jnp.bfloat16), axis_name, scatter_dimension=0, tiled=True
    ).astype(jnp.float32)


def pair_major(query, key, value, wide):
    pairs = query.shape[1] // wide
    return [
        part[:, j * wide : (j + 1) * wide] for j in range(pairs) for part in (query, key, value)
    ]


def from_pair_major(joined, wide):
    pairs = joined.shape[1] // (3 * wide)
    return [
        jnp.concatenate(
            [joined[:, (3 * j + i) * wide : (3 * j + i + 1) * wide] for j in range(pairs)], axis=1
        )
        for i in range(3)
    ]


def per_device(
    tokens,
    attn_gain,
    w_query,
    w_key,
    w_value,
    w_outgate,
    w_forget,
    forget_bias,
    w_output,
    query_gain,
    key_gain,
    mlp_gain,
    w_gate,
    w_up,
    w_down,
    lengths,
    out_grad,
):
    tensor_count = lax.axis_size("tensor")
    tensor_index = lax.axis_index("tensor")
    data_index = lax.axis_index("dp")
    local_rows = tokens.shape[0]
    slot = local_rows * tensor_count
    heads = w_forget.shape[1]
    half = query_gain.shape[0]
    wide = 2 * half
    width = heads * half
    hidden_width = w_gate.shape[1]
    shard = attn_gain.shape[0]
    length = lengths[0]

    small = jnp.concatenate(
        [
            w_forget,
            attn_gain[:, None],
            mlp_gain[:, None],
            jnp.zeros((shard, wide - heads - 2), jnp.bfloat16),
        ],
        axis=1,
    )
    first_full = gather(
        jnp.concatenate(pair_major(w_query, w_key, w_value, wide) + [small], axis=1), "dp"
    )
    second_full = gather(jnp.concatenate([w_outgate, w_output.T], axis=1), "dp")
    third_full = gather(jnp.concatenate([w_gate, w_up, w_down.T], axis=1), "dp")
    qkv_full = first_full[:, : 3 * width]
    small_full = first_full[:, 3 * width :]
    gain_one = small_full[:, heads].astype(jnp.float32)
    gain_two = small_full[:, heads + 1].astype(jnp.float32)
    outgate_full = second_full[:, :width]
    output_turned = second_full[:, width:]
    gate_full = third_full[:, :hidden_width]
    up_full = third_full[:, hidden_width : 2 * hidden_width]
    down_turned = third_full[:, 2 * hidden_width :]

    rows_float = tokens.astype(jnp.float32)
    scale_one = rms_scale(rows_float)
    normed_low = (rows_float * scale_one * gain_one).astype(jnp.bfloat16)
    normed_all = gather(normed_low, "tensor")
    projected = nn(normed_all, first_full)
    gate_logit = nn(normed_all, outgate_full)
    bias_local = lax.dynamic_slice_in_dim(forget_bias, tensor_index * heads, heads, 0)
    forget_logit = projected[:, 3 * width : 3 * width + heads] + bias_local[None, :]
    cumulative = jnp.cumsum(jax.nn.log_sigmoid(forget_logit), axis=0)
    query_pieces, key_pieces = bias_pieces(cumulative, length, slot, heads, wide)
    query_gain_wide = jnp.tile(query_gain.astype(jnp.float32), 2)[None]
    key_gain_wide = jnp.tile(key_gain.astype(jnp.float32), 2)[None]
    attended, query_feature, key_feature = attend(
        projected, query_pieces, key_pieces, query_gain_wide, key_gain_wide, heads, half
    )
    gate_open = jax.nn.sigmoid(gate_logit)
    gated_low = (attended * gate_open).astype(jnp.bfloat16)
    mixed = rows_float + scatter(nt(gated_low, output_turned), "tensor")

    scale_two = rms_scale(mixed)
    normed_mid = (mixed * scale_two * gain_two).astype(jnp.bfloat16)
    mid_all = gather(normed_mid, "tensor")
    gate_value = nn(mid_all, gate_full)
    up_value = nn(mid_all, up_full)
    gate_sigmoid = jax.nn.sigmoid(gate_value)
    gate_silu = gate_value * gate_sigmoid
    hidden_low = (gate_silu * up_value).astype(jnp.bfloat16)
    mixed_out = (mixed + scatter(nt(hidden_low, down_turned), "tensor")).astype(jnp.bfloat16)

    live_rows = tensor_index * local_rows + jnp.arange(local_rows) < length
    grad_out = jnp.where(live_rows[:, None], out_grad, jnp.zeros_like(out_grad))
    grad_out_all = gather(grad_out, "tensor")
    grad_hidden = nn(grad_out_all, down_turned)
    grad_down = tn(grad_out_all, hidden_low).astype(jnp.bfloat16)
    grad_gate_low = (
        grad_hidden * up_value * gate_sigmoid * (1.0 + gate_value * (1.0 - gate_sigmoid))
    ).astype(jnp.bfloat16)
    grad_up_low = (grad_hidden * gate_silu).astype(jnp.bfloat16)
    grad_mid = scatter(nt(grad_gate_low, gate_full) + nt(grad_up_low, up_full), "tensor")
    grad_gate_w = tn(mid_all, grad_gate_low).astype(jnp.bfloat16)
    grad_up_w = tn(mid_all, grad_up_low).astype(jnp.bfloat16)
    grad_gain_two = jnp.sum(grad_mid * mixed * scale_two, axis=0)
    grad_mixed = grad_out.astype(jnp.float32) + norm_backward(mixed, scale_two, grad_mid * gain_two)
    grad_mixed_all = gather(grad_mixed.astype(jnp.bfloat16), "tensor")
    grad_third = jnp.concatenate([grad_gate_w, grad_up_w, grad_down], axis=1)
    grad_third, grad_mixed_all = lax.optimization_barrier((grad_third, grad_mixed_all))
    third_sum = scatter(grad_third, "dp")

    grad_output_w = tn(grad_mixed_all, gated_low).astype(jnp.bfloat16)
    grad_gated = nn(grad_mixed_all, output_turned)
    grad_attended_low = (grad_gated * gate_open).astype(jnp.bfloat16)
    grad_gate_logit_low = (grad_gated * attended * gate_open * (1.0 - gate_open)).astype(
        jnp.bfloat16
    )
    grad_outgate_w = tn(normed_all, grad_gate_logit_low).astype(jnp.bfloat16)
    grad_qkv, grad_cumulative, gain_sums = attend_back(
        projected,
        query_feature,
        key_feature,
        attended,
        grad_attended_low,
        query_gain_wide,
        key_gain_wide,
        heads,
        half,
    )
    grad_log_forget = jnp.cumsum(grad_cumulative[::-1, :heads], axis=0)[::-1]
    grad_forget_low = (grad_log_forget * jax.nn.sigmoid(-forget_logit)).astype(jnp.bfloat16)
    grad_forget_wide = jnp.pad(grad_forget_low, ((0, 0), (0, wide - heads)))
    grad_bias_local = jnp.sum(grad_forget_low.astype(jnp.float32), axis=0)
    grad_normed = scatter(
        nt(grad_qkv, qkv_full)
        + nt(grad_gate_logit_low, outgate_full)
        + nt(grad_forget_wide, small_full),
        "tensor",
    )
    grad_first = jnp.concatenate(
        [
            tn(normed_all, grad_qkv).astype(jnp.bfloat16),
            tn(normed_all, grad_forget_wide).astype(jnp.bfloat16),
            grad_outgate_w,
            grad_output_w,
        ],
        axis=1,
    )
    first_sum = scatter(grad_first, "dp")
    grad_gain_one = jnp.sum(grad_normed * rows_float * scale_one, axis=0)
    tokens_grad = grad_mixed + norm_backward(rows_float, scale_one, grad_normed * gain_one)
    bias_spread = lax.dynamic_update_slice_in_dim(
        jnp.zeros(forget_bias.shape, jnp.float32), grad_bias_local, tensor_index * heads, 0
    )
    gain_one_sum, gain_two_sum, query_sum, key_sum, bias_sum = lax.psum(
        (grad_gain_one, grad_gain_two, gain_sums[0, :half], gain_sums[1, :half], bias_spread),
        ("dp", "tensor"),
    )
    own = data_index * shard
    grad_query_w, grad_key_w, grad_value_w = from_pair_major(first_sum[:, : 3 * width], wide)
    after = 3 * width + wide
    return (
        mixed_out,
        tokens_grad,
        lax.dynamic_slice_in_dim(gain_one_sum, own, shard, 0),
        grad_query_w,
        grad_key_w,
        grad_value_w,
        first_sum[:, after : after + width],
        first_sum[:, 3 * width : 3 * width + heads],
        bias_sum,
        first_sum[:, after + width :].T,
        query_sum,
        key_sum,
        lax.dynamic_slice_in_dim(gain_two_sum, own, shard, 0),
        third_sum[:, :hidden_width],
        third_sum[:, hidden_width : 2 * hidden_width],
        third_sum[:, 2 * hidden_width :].T,
    )


def solution(mesh):
    in_specs = (
        P(("dp", "tensor"), None),
        P("dp"),
        P("dp", "tensor"),
        P("dp", "tensor"),
        P("dp", "tensor"),
        P("dp", "tensor"),
        P("dp", "tensor"),
        P(),
        P("tensor", "dp"),
        P(),
        P(),
        P("dp"),
        P("dp", "tensor"),
        P("dp", "tensor"),
        P("tensor", "dp"),
        P("dp"),
        P(("dp", "tensor"), None),
    )
    out_specs = (
        P(("dp", "tensor"), None),
        P(("dp", "tensor"), None),
        P("dp"),
        P("dp", "tensor"),
        P("dp", "tensor"),
        P("dp", "tensor"),
        P("dp", "tensor"),
        P("dp", "tensor"),
        P(),
        P("tensor", "dp"),
        P(),
        P(),
        P("dp"),
        P("dp", "tensor"),
        P("dp", "tensor"),
        P("tensor", "dp"),
    )
    return jax.shard_map(
        per_device, mesh=mesh, in_specs=in_specs, out_specs=out_specs, check_vma=False
    )
```

```python
import functools
import math

import jax
import jax.numpy as jnp
from jax import lax
from jax.experimental import pallas as pl
from jax.experimental.pallas import tpu as pltpu
from jax.sharding import PartitionSpec as P

NEGATIVE = -1e30
EPSILON = 1e-05


def nt(left, right):
    return lax.dot_general(
        left, right, (((1,), (1,)), ((), ())), preferred_element_type=jnp.float32
    )


def tn(left, right):
    return lax.dot_general(
        left, right, (((0,), (0,)), ((), ())), preferred_element_type=jnp.float32
    )


def nn(left, right):
    return jnp.dot(left, right, preferred_element_type=jnp.float32)


def split_three(values):
    high = values.astype(jnp.bfloat16).astype(jnp.float32)
    rest = values - high
    middle = rest.astype(jnp.bfloat16).astype(jnp.float32)
    return high, middle, rest - middle


def placed_pieces(values, lane, first):
    high, middle, low = split_three(values)
    return jnp.where(
        lane == first, high, jnp.where(lane == first + 1, middle, jnp.where(lane == first + 2, low, 0.0))
    )


def turned(values, head, half):
    return values if head == 0 else pltpu.roll(values, half, 1)


def attend_kernel(
    heads, half, block, x_ref, cq_ref, ck_ref, qg_ref, kg_ref, att_ref, qb_ref, kf_ref, qf, vf
):
    pair = pl.program_id(0)
    slot = x_ref.shape[0]
    wide = 2 * half
    blocks = slot // block
    lane = lax.broadcasted_iota(jnp.int32, (block, wide), 1)
    lower = lane < half
    row = lax.broadcasted_iota(jnp.int32, (wide, wide), 0)
    col = lax.broadcasted_iota(jnp.int32, (wide, wide), 1)
    below = lax.broadcasted_iota(jnp.int32, (block, block), 0) >= lax.broadcasted_iota(
        jnp.int32, (block, block), 1
    )
    for h in range(2):
        head = pair * 2 + h
        place_q = ((row == (col - half) * heads + head) & (col >= half) & (col < half + 3)).astype(
            jnp.bfloat16
        )
        place_k = (
            (row == (col - half - 3) * heads + head) & (col >= half + 3) & (col < half + 6)
        ).astype(jnp.bfloat16)

        def prepare(b, _):
            rows = pl.ds(pl.multiple_of(b * block, block), block)
            q = turned(x_ref[rows, 0:wide], h, half)
            k = turned(x_ref[rows, wide : 2 * wide], h, half)
            v = turned(x_ref[rows, 2 * wide : 3 * wide], h, half)
            q_scale = lax.rsqrt(
                jnp.sum(jnp.where(lower, q * q, 0.0), axis=1, keepdims=True) / half + EPSILON
            )
            k_scale = lax.rsqrt(
                jnp.sum(jnp.where(lower, k * k, 0.0), axis=1, keepdims=True) / half + EPSILON
            )
            q_low = (q * q_scale * qg_ref[...]).astype(jnp.bfloat16).astype(jnp.float32)
            k_low = k * k_scale * kg_ref[...]
            q_bias = nn(cq_ref[rows, :], place_q) + jnp.where(
                (lane >= half + 3) & (lane < half + 6), 1.0, 0.0
            )
            k_bias = nn(ck_ref[rows, :], place_k) + jnp.where(
                (lane >= half) & (lane < half + 3), 1.0, 0.0
            )
            qf[rows, :] = jnp.where(lower, q_low * (1.0 / math.sqrt(half)), q_bias).astype(
                jnp.bfloat16
            )
            kf_ref[h, rows, :] = jnp.where(lower, k_low, k_bias).astype(jnp.bfloat16)
            vf[rows, :] = jnp.where(lower, v, 1.0).astype(jnp.bfloat16)
            return 0

        lax.fori_loop(0, blocks, prepare, 0)
        for qb in range(blocks):
            rows = pl.ds(qb * block, block)
            query = qf[rows, :]
            total = jnp.zeros((block, wide), jnp.float32)
            for kb in range(qb + 1):
                keys = pl.ds(kb * block, block)
                scores = nt(query, kf_ref[h, keys, :])
                if kb == qb:
                    scores = jnp.where(below, scores, NEGATIVE)
                total = total + nn(jnp.exp(scores).astype(jnp.bfloat16), vf[keys, :])
            out = total / pltpu.roll(total, half, 1)
            if h == 0:
                att_ref[rows, :] = out
            else:
                att_ref[rows, :] = jnp.where(lower, att_ref[rows, :], pltpu.roll(out, half, 1))
            query_float = query.astype(jnp.float32)
            bias = jnp.sum(
                jnp.where((lane >= half) & (lane < half + 3), query_float, 0.0),
                axis=1,
                keepdims=True,
            )
            shifted = bias - jnp.log(jnp.where(lower, 1.0, total))
            qb_ref[h, rows, :] = jnp.where(
                (lane >= half) & (lane < half + 3),
                placed_pieces(shifted, lane, half),
                query_float,
            ).astype(jnp.bfloat16)


def attend_back_kernel(
    half,
    block,
    x_ref,
    qb_ref,
    kf_ref,
    att_ref,
    do_ref,
    qg_ref,
    kg_ref,
    grad_ref,
    cum_ref,
    gain_ref,
    vf,
    dof,
    key_turned,
    dq_turned,
    dk_all,
    dv_all,
):
    pair = pl.program_id(0)
    slot = x_ref.shape[0]
    wide = 2 * half
    blocks = slot // block
    lane = lax.broadcasted_iota(jnp.int32, (block, wide), 1)
    lower = lane < half
    above = lax.broadcasted_iota(jnp.int32, (block, block), 0) <= lax.broadcasted_iota(
        jnp.int32, (block, block), 1
    )

    @pl.when(pair == 0)
    def _():
        gain_ref[...] = jnp.zeros_like(gain_ref)
        cum_ref[...] = jnp.zeros_like(cum_ref)

    for h in range(2):
        head = pair * 2 + h

        def prepare(b, _):
            rows = pl.ds(pl.multiple_of(b * block, block), block)
            v = turned(x_ref[rows, 2 * wide : 3 * wide], h, half)
            grad = turned(do_ref[rows, :].astype(jnp.float32), h, half)
            out = turned(att_ref[rows, :], h, half)
            inner = jnp.sum(jnp.where(lower, grad * out, 0.0), axis=1, keepdims=True)
            vf[rows, :] = jnp.where(lower, v, 1.0).astype(jnp.bfloat16)
            dof[rows, :] = jnp.where(lower, grad, placed_pieces(-inner, lane, half)).astype(
                jnp.bfloat16
            )
            key_turned[:, rows] = kf_ref[h, rows, :].astype(jnp.float32).T.astype(jnp.bfloat16)
            return 0

        lax.fori_loop(0, blocks, prepare, 0)
        for kb in range(blocks):
            keys = pl.ds(kb * block, block)
            key = kf_ref[h, keys, :]
            value = vf[keys, :]
            dk = jnp.zeros((block, wide), jnp.float32)
            dv = jnp.zeros((block, wide), jnp.float32)
            for qb in range(kb, blocks):
                rows = pl.ds(qb * block, block)
                query = qb_ref[h, rows, :]
                grad = dof[rows, :]
                scores = nt(key, query)
                if kb == qb:
                    scores = jnp.where(above, scores, NEGATIVE)
                probs = jnp.exp(scores)
                dv = dv + nn(probs.astype(jnp.bfloat16), grad)
                grad_scores = (probs * nt(value, grad)).astype(jnp.bfloat16)
                dk = dk + nn(grad_scores, query)
                part = nn(key_turned[:, keys], grad_scores)
                if kb == 0:
                    dq_turned[:, rows] = part
                else:
                    dq_turned[:, rows] += part
            dk_all[keys, :] = dk
            dv_all[keys, :] = dv

        def finish(b, sums):
            rows = pl.ds(pl.multiple_of(b * block, block), block)
            dq = dq_turned[:, rows].T
            dk = dk_all[rows, :]
            change = jnp.sum(
                jnp.where(lane == half, dq - pltpu.roll(dk, wide - 3, 1), 0.0),
                axis=1,
                keepdims=True,
            )
            cum_ref[rows, :] = jnp.where(lane == head, change, cum_ref[rows, :])

            def one(raw, grad, gain):
                scale = lax.rsqrt(
                    jnp.sum(jnp.where(lower, raw * raw, 0.0), axis=1, keepdims=True) / half
                    + EPSILON
                )
                inward = grad * gain
                mean = (
                    jnp.sum(jnp.where(lower, inward * raw, 0.0), axis=1, keepdims=True) / half
                )
                out = scale * inward - raw * (scale * scale * scale) * mean
                return out, jnp.sum(grad * raw * scale, axis=0, keepdims=True)

            q_out, q_sum = one(
                turned(x_ref[rows, 0:wide], h, half), dq * (1.0 / math.sqrt(half)), qg_ref[...]
            )
            k_out, k_sum = one(turned(x_ref[rows, wide : 2 * wide], h, half), dk, kg_ref[...])
            v_out = dv_all[rows, :]
            for i, out in enumerate((q_out, k_out, v_out)):
                at = slice(i * wide, (i + 1) * wide)
                if h == 0:
                    grad_ref[rows, at] = out.astype(jnp.bfloat16)
                else:
                    grad_ref[rows, at] = jnp.where(
                        lower, grad_ref[rows, at].astype(jnp.float32), pltpu.roll(out, half, 1)
                    ).astype(jnp.bfloat16)
            return sums[0] + q_sum, sums[1] + k_sum

        zero = jnp.zeros((1, wide), jnp.float32)
        q_sum, k_sum = lax.fori_loop(0, blocks, finish, (zero, zero))
        gain_ref[0:1, :] += q_sum
        gain_ref[1:2, :] += k_sum


def attend(x, cq, ck, q_gain, k_gain, heads, half):
    slot = x.shape[0]
    wide = 2 * half
    pairs = heads // 2
    block = min(512, slot)
    constant = lambda rows: pl.BlockSpec((rows, wide), lambda j: (0, 0))
    area = slot * (slot + block) // 2
    return pl.pallas_call(
        functools.partial(attend_kernel, heads, half, block),
        grid=(pairs,),
        in_specs=[
            pl.BlockSpec((slot, 3 * wide), lambda j: (0, j)),
            constant(slot),
            constant(slot),
            constant(1),
            constant(1),
        ],
        out_specs=[
            pl.BlockSpec((slot, wide), lambda j: (0, j)),
            pl.BlockSpec((2, slot, wide), lambda j: (j, 0, 0)),
            pl.BlockSpec((2, slot, wide), lambda j: (j, 0, 0)),
        ],
        out_shape=[
            jax.ShapeDtypeStruct((slot, pairs * wide), jnp.float32),
            jax.ShapeDtypeStruct((heads, slot, wide), jnp.bfloat16),
            jax.ShapeDtypeStruct((heads, slot, wide), jnp.bfloat16),
        ],
        scratch_shapes=[pltpu.VMEM((slot, wide), jnp.bfloat16)] * 2,
        cost_estimate=pl.CostEstimate(
            flops=4 * heads * area * wide,
            transcendentals=heads * area,
            bytes_accessed=slot * pairs * wide * 24,
        ),
        name="attend",
    )(x, cq, ck, q_gain, k_gain)


def attend_back(x, qb, kf, att, grad, q_gain, k_gain, heads, half):
    slot = x.shape[0]
    wide = 2 * half
    pairs = heads // 2
    block = min(512, slot)
    area = slot * (slot + block) // 2
    gain = pl.BlockSpec((1, wide), lambda j: (0, 0))
    tall = pl.BlockSpec((2, slot, wide), lambda j: (j, 0, 0))
    column = pl.BlockSpec((slot, wide), lambda j: (0, j))
    return pl.pallas_call(
        functools.partial(attend_back_kernel, half, block),
        grid=(pairs,),
        in_specs=[
            pl.BlockSpec((slot, 3 * wide), lambda j: (0, j)),
            tall,
            tall,
            column,
            column,
            gain,
            gain,
        ],
        out_specs=[
            pl.BlockSpec((slot, 3 * wide), lambda j: (0, j)),
            pl.BlockSpec((slot, wide), lambda j: (0, 0)),
            pl.BlockSpec((8, wide), lambda j: (0, 0)),
        ],
        out_shape=[
            jax.ShapeDtypeStruct((slot, 3 * pairs * wide), jnp.bfloat16),
            jax.ShapeDtypeStruct((slot, wide), jnp.float32),
            jax.ShapeDtypeStruct((8, wide), jnp.float32),
        ],
        scratch_shapes=[
            pltpu.VMEM((slot, wide), jnp.bfloat16),
            pltpu.VMEM((slot, wide), jnp.bfloat16),
            pltpu.VMEM((wide, slot), jnp.bfloat16),
            pltpu.VMEM((wide, slot), jnp.float32),
            pltpu.VMEM((slot, wide), jnp.float32),
            pltpu.VMEM((slot, wide), jnp.float32),
        ],
        cost_estimate=pl.CostEstimate(
            flops=10 * heads * area * wide,
            transcendentals=heads * area,
            bytes_accessed=slot * pairs * wide * 40,
        ),
        name="attend_back",
    )(x, qb, kf, att, grad, q_gain, k_gain)


def tensor_peers():
    me = lax.axis_index("tensor")
    partner = me + 1 - 2 * lax.rem(me, 2)
    across = lax.rem(me + 2, 4)
    return me, partner, across, lax.rem(partner + 2, 4)


def greet(names):
    barrier = pltpu.get_barrier_semaphore()
    for name in names:
        pl.semaphore_signal(barrier, inc=1, device_id=name, device_id_type=pl.DeviceIdType.MESH)
    pl.semaphore_wait(barrier, len(names))


def send(source, target, sent, received, name):
    return pltpu.make_async_remote_copy(
        src_ref=source,
        dst_ref=target,
        send_sem=sent,
        recv_sem=received,
        device_id=name,
        device_id_type=pl.DeviceIdType.MESH,
    )


def gather_kernel(count, chunks, *refs):
    ins, outs = refs[:count], refs[count : 2 * count]
    kept, near_out, near_in, far_out, far_in, pass_out, pass_in = refs[2 * count :]
    me, partner, across, _ = tensor_peers()
    greet(({"tensor": partner}, {"tensor": across}))
    rows = ins[0].shape[0]
    step = rows // chunks

    def place(owner, c):
        return pl.ds(pl.multiple_of(owner * rows + c * step, step), step)

    own = pl.ds(pl.multiple_of(me * rows, rows), rows)
    far, near, local, passed = [], [], [], []
    for i in range(count):
        for c in range(chunks):
            far.append(
                send(
                    ins[i].at[pl.ds(c * step, step)],
                    outs[i].at[place(me, c)],
                    far_out.at[i, c],
                    far_in.at[i, c],
                    {"tensor": across},
                )
            )
            far[-1].start()
    for i in range(count):
        near.append(
            send(ins[i], outs[i].at[own], near_out.at[i], near_in.at[i], {"tensor": partner})
        )
        near[-1].start()
        local.append(pltpu.make_async_copy(ins[i], outs[i].at[own], kept.at[i]))
        local[-1].start()
    for i in range(count):
        for c in range(chunks):
            far[i * chunks + c].wait_recv()
            passed.append(
                send(
                    outs[i].at[place(across, c)],
                    outs[i].at[place(across, c)],
                    pass_out.at[i, c],
                    pass_in.at[i, c],
                    {"tensor": partner},
                )
            )
            passed[-1].start()
    for copy in local + near + passed:
        copy.wait()
    for copy in far:
        copy.wait_send()


def tensor_gather(arrays, number):
    count, chunks = len(arrays), 4
    rows, columns = arrays[0].shape
    moved = count * rows * columns * 2
    return pl.pallas_call(
        functools.partial(gather_kernel, count, chunks),
        in_specs=[pl.BlockSpec(memory_space=pltpu.VMEM)] * count,
        out_specs=[pl.BlockSpec(memory_space=pl.ANY)] * count,
        out_shape=[jax.ShapeDtypeStruct((4 * rows, columns), a.dtype) for a in arrays],
        scratch_shapes=[
            pltpu.SemaphoreType.DMA((count,)),
            pltpu.SemaphoreType.DMA((count,)),
            pltpu.SemaphoreType.DMA((count,)),
        ]
        + [pltpu.SemaphoreType.DMA((count, chunks))] * 4,
        compiler_params=pltpu.CompilerParams(collective_id=number, has_side_effects=True),
        cost_estimate=pl.CostEstimate(flops=0, transcendentals=0, bytes_accessed=80 * moved),
        name="tensor_gather",
    )(*arrays)


def scatter_kernel(
    chunks, p_ref, o_ref, given, own_in, outgoing, arriving, near_out, near_in, own_out, own_sem, far_out, far_in
):
    me, partner, across, opposite = tensor_peers()
    greet(({"tensor": partner}, {"tensor": across}))
    rows = o_ref.shape[0]
    step = rows // chunks

    def place(owner, c):
        return pl.ds(pl.multiple_of(owner * rows + c * step, step), step)

    near, far = [], []
    for c in range(chunks):
        near.append(
            send(
                p_ref.at[place(opposite, c)],
                given.at[pl.ds(c * step, step)],
                near_out.at[c],
                near_in.at[c],
                {"tensor": partner},
            )
        )
        near[-1].start()
    own = send(
        p_ref.at[pl.ds(pl.multiple_of(partner * rows, rows), rows)],
        own_in,
        own_out,
        own_sem,
        {"tensor": partner},
    )
    own.start()
    for c in range(chunks):
        near[c].wait_recv()
        part = pl.ds(c * step, step)
        outgoing[part, :] = (
            p_ref[place(across, c), :].astype(jnp.float32) + given[part, :].astype(jnp.float32)
        ).astype(outgoing.dtype)
        far.append(
            send(
                outgoing.at[part], arriving.at[part], far_out.at[c], far_in.at[c], {"tensor": across}
            )
        )
        far[-1].start()
    own.wait_recv()
    for c in range(chunks):
        far[c].wait_recv()
        part = pl.ds(c * step, step)
        o_ref[part, :] = (
            p_ref[place(me, c), :].astype(jnp.float32)
            + own_in[part, :].astype(jnp.float32)
            + arriving[part, :].astype(jnp.float32)
        )
    own.wait_send()
    for copy in near + far:
        copy.wait_send()


def tensor_scatter(values, number):
    chunks = 4
    rows, columns = values.shape[0] // 4, values.shape[1]
    block = pltpu.VMEM((rows, columns), values.dtype)
    return pl.pallas_call(
        functools.partial(scatter_kernel, chunks),
        in_specs=[pl.BlockSpec(memory_space=pltpu.VMEM)],
        out_specs=pl.BlockSpec(memory_space=pltpu.VMEM),
        out_shape=jax.ShapeDtypeStruct((rows, columns), jnp.float32),
        scratch_shapes=[block] * 4
        + [pltpu.SemaphoreType.DMA((chunks,))] * 2
        + [pltpu.SemaphoreType.DMA(())] * 2
        + [pltpu.SemaphoreType.DMA((chunks,))] * 2,
        compiler_params=pltpu.CompilerParams(collective_id=number, has_side_effects=True),
        cost_estimate=pl.CostEstimate(
            flops=0, transcendentals=0, bytes_accessed=80 * rows * columns * 2
        ),
        name="tensor_scatter",
    )(values)


def sum_kernel(data_count, x_ref, o_ref, near_all, far_all, near_out, near_in, far_out, far_in):
    me = lax.axis_index("tensor")
    data = lax.axis_index("dp")
    near_names = [{"tensor": lax.rem(me + k, 4)} for k in range(1, 4)]
    far_names = [{"dp": lax.rem(data + k, data_count)} for k in range(1, data_count)]
    greet(near_names + far_names)
    copies = []
    for k, name in enumerate(near_names):
        copies.append(send(x_ref, near_all.at[me], near_out.at[k], near_in.at[k], name))
        copies[-1].start()
    near_all[me] = x_ref[...]
    for copy in copies:
        copy.wait()
    o_ref[...] = near_all[0] + near_all[1] + near_all[2] + near_all[3]
    copies = []
    for k, name in enumerate(far_names):
        copies.append(send(o_ref, far_all.at[data], far_out.at[k], far_in.at[k], name))
        copies[-1].start()
    far_all[data] = o_ref[...]
    for copy in copies:
        copy.wait()
    o_ref[...] = jnp.sum(far_all[...], axis=0)


def sum_all(values, number):
    data_count = lax.axis_size("dp")
    return pl.pallas_call(
        functools.partial(sum_kernel, data_count),
        in_specs=[pl.BlockSpec(memory_space=pltpu.VMEM)],
        out_specs=pl.BlockSpec(memory_space=pltpu.VMEM),
        out_shape=jax.ShapeDtypeStruct(values.shape, jnp.float32),
        scratch_shapes=[
            pltpu.VMEM((4,) + values.shape, jnp.float32),
            pltpu.VMEM((data_count,) + values.shape, jnp.float32),
            pltpu.SemaphoreType.DMA((3,)),
            pltpu.SemaphoreType.DMA((3,)),
            pltpu.SemaphoreType.DMA((data_count - 1,)),
            pltpu.SemaphoreType.DMA((data_count - 1,)),
        ],
        compiler_params=pltpu.CompilerParams(collective_id=number, has_side_effects=True),
        cost_estimate=pl.CostEstimate(flops=0, transcendentals=0, bytes_accessed=30_000_000),
        name="sum_all",
    )(values)


def split_pieces(values):
    high = lax.reduce_precision(values, 8, 7)
    middle = lax.reduce_precision(values - high, 8, 7)
    return high, middle, lax.reduce_precision(values - high - middle, 8, 7)


def bias_pieces(cumulative, length, slot, heads, wide):
    live = (jnp.arange(slot) < length)[:, None]
    last = lax.dynamic_slice_in_dim(cumulative, length - 1, 1, 0)
    query_side = jnp.where(live, cumulative, last)
    pad = jnp.zeros((slot, wide - 3 * heads), jnp.float32)
    high, middle, low = split_pieces(-cumulative)
    key_side = (jnp.where(live, high, NEGATIVE), jnp.where(live, middle, 0.0), jnp.where(live, low, 0.0))
    return (
        jnp.concatenate(split_pieces(query_side) + (pad,), axis=1).astype(jnp.bfloat16),
        jnp.concatenate(key_side + (pad,), axis=1).astype(jnp.bfloat16),
    )


def rms_scale(values):
    return lax.rsqrt(jnp.mean(values * values, axis=-1, keepdims=True) + EPSILON)


def norm_backward(values, scaling, grad_normed):
    cubed = scaling * scaling * scaling
    return scaling * grad_normed - values * cubed * jnp.mean(
        grad_normed * values, axis=-1, keepdims=True
    )


def gather(values, axis_name):
    return lax.all_gather(values, axis_name, axis=0, tiled=True)


def scatter(values, axis_name):
    return lax.psum_scatter(
        values.astype(jnp.bfloat16), axis_name, scatter_dimension=0, tiled=True
    ).astype(jnp.float32)


def pair_major(query, key, value, wide):
    pairs = query.shape[1] // wide
    return [
        part[:, j * wide : (j + 1) * wide] for j in range(pairs) for part in (query, key, value)
    ]


def from_pair_major(joined, wide):
    pairs = joined.shape[1] // (3 * wide)
    return [
        jnp.concatenate(
            [joined[:, (3 * j + i) * wide : (3 * j + i + 1) * wide] for j in range(pairs)], axis=1
        )
        for i in range(3)
    ]


def per_device(
    tokens,
    attn_gain,
    w_query,
    w_key,
    w_value,
    w_outgate,
    w_forget,
    forget_bias,
    w_output,
    query_gain,
    key_gain,
    mlp_gain,
    w_gate,
    w_up,
    w_down,
    lengths,
    out_grad,
):
    tensor_count = lax.axis_size("tensor")
    tensor_index = lax.axis_index("tensor")
    data_index = lax.axis_index("dp")
    local_rows = tokens.shape[0]
    slot = local_rows * tensor_count
    heads = w_forget.shape[1]
    half = query_gain.shape[0]
    wide = 2 * half
    width = heads * half
    hidden_width = w_gate.shape[1]
    shard = attn_gain.shape[0]
    length = lengths[0]

    small = jnp.concatenate(
        [
            w_forget,
            attn_gain[:, None],
            mlp_gain[:, None],
            jnp.zeros((shard, wide - heads - 2), jnp.bfloat16),
        ],
        axis=1,
    )
    first_full = gather(
        jnp.concatenate(pair_major(w_query, w_key, w_value, wide) + [small], axis=1), "dp"
    )
    second_full = gather(jnp.concatenate([w_outgate, w_output.T], axis=1), "dp")
    third_full = gather(jnp.concatenate([w_gate, w_up], axis=1), "dp")
    down_turned = gather(w_down.T, "dp")
    qkv_full = first_full[:, : 3 * width]
    small_full = first_full[:, 3 * width :]
    gain_one = small_full[:, heads].astype(jnp.float32)
    gain_two = small_full[:, heads + 1].astype(jnp.float32)
    outgate_full = second_full[:, :width]
    output_turned = second_full[:, width:]
    gate_full = third_full[:, :hidden_width]
    up_full = third_full[:, hidden_width:]

    tokens_all, out_grad_all = tensor_gather((tokens, out_grad), 0)
    tokens_all_float = tokens_all.astype(jnp.float32)
    normed_all = (tokens_all_float * rms_scale(tokens_all_float) * gain_one).astype(jnp.bfloat16)
    rows_float = tokens.astype(jnp.float32)
    scale_one = rms_scale(rows_float)
    projected = nn(normed_all, first_full)
    gate_logit = nn(normed_all, outgate_full)
    bias_local = lax.dynamic_slice_in_dim(forget_bias, tensor_index * heads, heads, 0)
    forget_logit = projected[:, 3 * width : 3 * width + heads] + bias_local[None, :]
    cumulative = jnp.cumsum(jax.nn.log_sigmoid(forget_logit), axis=0)
    query_pieces, key_pieces = bias_pieces(cumulative, length, slot, heads, wide)
    query_gain_wide = jnp.tile(query_gain.astype(jnp.float32), 2)[None]
    key_gain_wide = jnp.tile(key_gain.astype(jnp.float32), 2)[None]
    attended, query_feature, key_feature = attend(
        projected, query_pieces, key_pieces, query_gain_wide, key_gain_wide, heads, half
    )
    gate_open = jax.nn.sigmoid(gate_logit)
    gated_low = (attended * gate_open).astype(jnp.bfloat16)
    mixed = rows_float + tensor_scatter(nt(gated_low, output_turned).astype(jnp.bfloat16), 1)

    scale_two = rms_scale(mixed)
    normed_mid = (mixed * scale_two * gain_two).astype(jnp.bfloat16)
    mid_all = tensor_gather((normed_mid,), 2)[0]
    gate_value = nn(mid_all, gate_full)
    up_value = nn(mid_all, up_full)
    gate_sigmoid = jax.nn.sigmoid(gate_value)
    gate_silu = gate_value * gate_sigmoid
    hidden_low = (gate_silu * up_value).astype(jnp.bfloat16)
    mixed_out = (mixed + scatter(nt(hidden_low, down_turned), "tensor")).astype(jnp.bfloat16)

    live_rows = tensor_index * local_rows + jnp.arange(local_rows) < length
    grad_out = jnp.where(live_rows[:, None], out_grad, jnp.zeros_like(out_grad))
    grad_out_all = jnp.where(
        jnp.arange(slot)[:, None] < length, out_grad_all, jnp.zeros_like(out_grad_all)
    )
    grad_hidden = nn(grad_out_all, down_turned)
    grad_down = tn(grad_out_all, hidden_low).astype(jnp.bfloat16)
    grad_gate_low = (
        grad_hidden * up_value * gate_sigmoid * (1.0 + gate_value * (1.0 - gate_sigmoid))
    ).astype(jnp.bfloat16)
    grad_up_low = (grad_hidden * gate_silu).astype(jnp.bfloat16)
    grad_mid = tensor_scatter(
        (nt(grad_gate_low, gate_full) + nt(grad_up_low, up_full)).astype(jnp.bfloat16), 1
    )
    grad_gate_w = tn(mid_all, grad_gate_low).astype(jnp.bfloat16)
    grad_up_w = tn(mid_all, grad_up_low).astype(jnp.bfloat16)
    grad_gain_two = jnp.sum(grad_mid * mixed * scale_two, axis=0)
    grad_mixed = grad_out.astype(jnp.float32) + norm_backward(mixed, scale_two, grad_mid * gain_two)
    grad_mixed_all = tensor_gather((grad_mixed.astype(jnp.bfloat16),), 2)[0]
    third_sum = scatter(jnp.concatenate([grad_gate_w, grad_up_w, grad_down], axis=1), "dp")

    grad_output_w = tn(grad_mixed_all, gated_low).astype(jnp.bfloat16)
    grad_gated = nn(grad_mixed_all, output_turned)
    grad_attended_low = (grad_gated * gate_open).astype(jnp.bfloat16)
    grad_gate_logit_low = (grad_gated * attended * gate_open * (1.0 - gate_open)).astype(
        jnp.bfloat16
    )
    grad_outgate_w = tn(normed_all, grad_gate_logit_low).astype(jnp.bfloat16)
    grad_qkv, grad_cumulative, gain_sums = attend_back(
        projected,
        query_feature,
        key_feature,
        attended,
        grad_attended_low,
        query_gain_wide,
        key_gain_wide,
        heads,
        half,
    )
    grad_log_forget = jnp.cumsum(grad_cumulative[::-1, :heads], axis=0)[::-1]
    grad_forget_low = (grad_log_forget * jax.nn.sigmoid(-forget_logit)).astype(jnp.bfloat16)
    grad_forget_wide = jnp.pad(grad_forget_low, ((0, 0), (0, wide - heads)))
    grad_bias_local = jnp.sum(grad_forget_low.astype(jnp.float32), axis=0)
    grad_normed = tensor_scatter(
        (
            nt(grad_qkv, qkv_full)
            + nt(grad_gate_logit_low, outgate_full)
            + nt(grad_forget_wide, small_full)
        ).astype(jnp.bfloat16),
        1,
    )
    grad_first = jnp.concatenate(
        [
            tn(normed_all, grad_qkv).astype(jnp.bfloat16),
            tn(normed_all, grad_forget_wide).astype(jnp.bfloat16),
            grad_outgate_w,
            grad_output_w,
        ],
        axis=1,
    )
    first_sum = scatter(grad_first, "dp")
    grad_gain_one = jnp.sum(grad_normed * rows_float * scale_one, axis=0)
    tokens_grad = grad_mixed + norm_backward(rows_float, scale_one, grad_normed * gain_one)
    bias_spread = lax.dynamic_update_slice_in_dim(
        jnp.zeros(forget_bias.shape, jnp.float32), grad_bias_local, tensor_index * heads, 0
    )
    parts = (grad_gain_one, grad_gain_two, gain_sums[0, :half], gain_sums[1, :half], bias_spread)
    joined = jnp.concatenate(parts)
    lines = -(-joined.shape[0] // (8 * wide)) * 8
    joined = jnp.pad(joined, (0, lines * wide - joined.shape[0])).reshape(lines, wide)
    joined = sum_all(joined, 3).reshape(-1)
    sums, start = [], 0
    for part in parts:
        sums.append(joined[start : start + part.shape[0]])
        start += part.shape[0]
    gain_one_sum, gain_two_sum, query_sum, key_sum, bias_sum = sums
    own = data_index * shard
    grad_query_w, grad_key_w, grad_value_w = from_pair_major(first_sum[:, : 3 * width], wide)
    after = 3 * width + wide
    return (
        mixed_out,
        tokens_grad,
        lax.dynamic_slice_in_dim(gain_one_sum, own, shard, 0),
        grad_query_w,
        grad_key_w,
        grad_value_w,
        first_sum[:, after : after + width],
        first_sum[:, 3 * width : 3 * width + heads],
        bias_sum,
        first_sum[:, after + width :].T,
        query_sum,
        key_sum,
        lax.dynamic_slice_in_dim(gain_two_sum, own, shard, 0),
        third_sum[:, :hidden_width],
        third_sum[:, hidden_width : 2 * hidden_width],
        third_sum[:, 2 * hidden_width :].T,
    )


def solution(mesh):
    in_specs = (
        P(("dp", "tensor"), None),
        P("dp"),
        P("dp", "tensor"),
        P("dp", "tensor"),
        P("dp", "tensor"),
        P("dp", "tensor"),
        P("dp", "tensor"),
        P(),
        P("tensor", "dp"),
        P(),
        P(),
        P("dp"),
        P("dp", "tensor"),
        P("dp", "tensor"),
        P("tensor", "dp"),
        P("dp"),
        P(("dp", "tensor"), None),
    )
    out_specs = (
        P(("dp", "tensor"), None),
        P(("dp", "tensor"), None),
        P("dp"),
        P("dp", "tensor"),
        P("dp", "tensor"),
        P("dp", "tensor"),
        P("dp", "tensor"),
        P("dp", "tensor"),
        P(),
        P("tensor", "dp"),
        P(),
        P(),
        P("dp"),
        P("dp", "tensor"),
        P("dp", "tensor"),
        P("tensor", "dp"),
    )
    return jax.shard_map(
        per_device, mesh=mesh, in_specs=in_specs, out_specs=out_specs, check_vma=False
    )
```
